32 devices in a mesh: dp: 8 (over z, x), head: 4 (over y, core).
Axes of the slice: x: 2, y: 2, z: 4, core: 2. Of those that a mesh axis runs over, the one named last changes fastest.
Arguments:
- inputs: bfloat16 [8192, 512], P(('dp', 'head')), may hold values from -6 to 6
- segments: int32 [32, 256], P('dp'), may hold values from 0 to 3, never falling along the last dimension, each value on 1 to 128 neighbouring positions
- cotangent: bfloat16 [8192, 512], P(('dp', 'head')), may hold values from -26 to 26
- first_gain: float32 [512], replicated, may hold values from 0.1 to 1.9
- first_bias: float32 [512], replicated, may hold values from -3 to 3
- project_in: bfloat16 [512, 3, 512], P(None, None, 'head'), may hold values from -0.25 to 0.25
- sort_weight: float32 [512, 8, 8], P(None, 'head'), may hold values from -1.5 to 1.5
- project_out: bfloat16 [512, 512], P('head'), may hold values from -1.5 to 1.5
- second_gain: float32 [512], replicated, may hold values from 0.1 to 1.9
- second_bias: float32 [512], replicated, may hold values from -3 to 3
- up_weight: bfloat16 [512, 2048], P(None, 'head'), may hold values from -0.25 to 0.25
- up_bias: float32 [2048], P('head'), may hold values from -3 to 3
- down_weight: bfloat16 [2048, 512], P('head'), may hold values from -0.125 to 0.125
- down_bias: float32 [512], replicated, may hold values from -3 to 3
Outputs:
- output: bfloat16 [8192, 512], P(('dp', 'head'))
- grad_inputs: bfloat16 [8192, 512], P(('dp', 'head'))
- grad_first_gain: float32 [512], replicated
- grad_first_bias: float32 [512], replicated
- grad_project_in: float32 [512, 3, 512], P(None, None, 'head')
- grad_sort_weight: float32 [512, 8, 8], P(None, 'head')
- grad_project_out: float32 [512, 512], P('head')
- grad_second_gain: float32 [512], replicated
- grad_second_bias: float32 [512], replicated
- grad_up_weight: float32 [512, 2048], P(None, 'head')
- grad_up_bias: float32 [2048], P('head')
- grad_down_weight: float32 [2048, 512], P('head')
- grad_down_bias: float32 [512], replicated
The draws below stay inside these ranges and needn't reach their ends.
Inputs may be any that keep to these rules, and one draw needn't show every extreme that they name: In every row segment numbers never fall; each of the 4 segments holds 1 to 128 tokens and one holds exactly 128.
All inputs are finite; a program needn't handle non-finite values.
Results may differ from the reference program's by a relative error of at most 0.018.
Values may be sent and summed in bfloat16 or wider, within the bound.
A program may use at most 128 MiB of HBM per device.

```python
import math
import jax
import jax.numpy as jnp
import numpy as np
from jax import lax

D = 512
HEADS = 8
FF = 2048
HEAD_DIM = 64
BLOCK = 32
NBLK = 8
LEN = 256
SINK_ITERS = 8
SEGS = 4
SEG_MOST = 128
ROWS = 32
TOKENS = 8192


def draw_cotangent(key, part):
    noise_part = jnp.clip(jax.random.normal(key, (TOKENS, D), jnp.float32), -6.0, 6.0)
    growth = 1.0 + 2.0 * jnp.arange(TOKENS, dtype=jnp.float32)[:, None] / TOKENS
    return (noise_part * growth).astype(jnp.bfloat16)


def block_levels(stream_key, dims, split, smallest, high):
    def one(dim, parts):
        draws = jax.random.uniform(jax.random.fold_in(jax.random.fold_in(stream_key, 6), dim), (parts,), jnp.float32, smallest / len(split), high / len(split))
        return jnp.repeat(jnp.exp(draws), dims[dim] // parts).reshape((-1,) + (1,) * (len(dims) - dim - 1))

    level = one(*split[0])
    for cut in split[1:]:
        level = level * one(*cut)
    return level


def profile(number_of, total, bound, skew):
    portions = [(1 << 20) // math.isqrt(grade ** skew) + 1 for grade in range(2, number_of + 1)]
    rest, counts = total - bound - (number_of - 1), [1] * (number_of - 1)
    while rest > 0:
        free = [i for i in range(number_of - 1) if counts[i] < bound]
        whole, left = sum([portions[i] for i in free]), rest
        for i in free:
            more = min(bound - counts[i], max(1, left * portions[i] // whole), rest)
            counts[i] = counts[i] + more
            rest = rest - more
    return np.array([bound] + counts)


def uneven(key, amount, total, most, slope):
    if amount == 2:
        one = jax.random.randint(key, (), max(1, total - most), min(most, total - 1) + 1)
        return jnp.stack([one, total - one])
    tallies = jnp.asarray(profile(amount, total, most, slope), jnp.int32)
    pairs = (amount - 1) // 2
    giver, receiver = tallies[1:1 + 2 * pairs:2], tallies[2:2 + 2 * pairs:2]
    room = jnp.minimum(giver - 1, most - receiver)
    shifted = jax.random.randint(jax.random.fold_in(key, 1), (pairs,), 0, 1 << 20) % (room + 1)
    tallies = tallies.at[1:1 + 2 * pairs:2].set(giver - shifted).at[2:2 + 2 * pairs:2].set(receiver + shifted)
    return tallies[jax.random.permutation(jax.random.fold_in(key, 2), amount)]


def centred(own_key, shape, deviation, most, split=(), held_as=jnp.bfloat16):
    gain = block_levels(own_key, shape, split, -0.22, 0.18) if split else 1.0
    drawn = jax.random.normal(own_key, shape, jnp.float32) * deviation * gain
    return jnp.minimum(jnp.maximum(drawn, -most), most).astype(held_as)


def setup_inputs(seed: int = 0) -> dict:
    arg_keys = jax.random.split(jax.random.key(seed), 15)
    inputs = centred(arg_keys[0], (TOKENS, D), 1.0, 6.0, ((0, 32),))
    segments = jax.vmap(lambda own: jnp.searchsorted(jnp.cumsum(uneven(own, SEGS, LEN, SEG_MOST, 1)), jnp.arange(LEN), side="right"))(jax.random.split(arg_keys[1], ROWS)).reshape((ROWS, LEN)).astype(jnp.int32)
    cotangent = draw_cotangent(jax.random.fold_in(arg_keys[14], 71), 0)
    first_gain = jnp.clip(1.0 + 0.18 * jax.random.normal(arg_keys[3], (D,), jnp.float32), 0.1, 1.9)
    first_bias = centred(arg_keys[4], (D,), 0.5, 3.0, (), jnp.float32)
    project_in = centred(arg_keys[5], (D, 3, D), D ** -0.5, 0.25, ((2, 4),))
    sort_weight = centred(arg_keys[6], (D, HEADS, NBLK), (D // 32) ** -0.5, 1.5, ((1, 4),), jnp.float32)
    project_out = centred(arg_keys[7], (D, D), (D // 32) ** -0.5, 1.5, ((0, 4),))
    second_gain = jnp.clip(1.0 + 0.18 * jax.random.normal(arg_keys[8], (D,), jnp.float32), 0.1, 1.9)
    second_bias = centred(arg_keys[9], (D,), 0.5, 3.0, (), jnp.float32)
    up_weight = centred(arg_keys[10], (D, FF), D ** -0.5, 0.25, ((1, 4),))
    up_bias = centred(arg_keys[11], (FF,), 0.5, 3.0, ((0, 4),), jnp.float32)
    down_weight = centred(arg_keys[12], (FF, D), FF ** -0.5, 0.125, ((0, 4),))
    down_bias = centred(arg_keys[13], (D,), 0.5, 3.0, (), jnp.float32)
    return dict(inputs=inputs, segments=segments, cotangent=cotangent, first_gain=first_gain, first_bias=first_bias, project_in=project_in, sort_weight=sort_weight, project_out=project_out, second_gain=second_gain, second_bias=second_bias, up_weight=up_weight, up_bias=up_bias, down_weight=down_weight, down_bias=down_bias)


@jax.custom_vjp
def low(v):
    return lax.optimization_barrier(v.astype(jnp.bfloat16)).astype(jnp.float32)

@jax.custom_vjp
def low_back(v):
    return v

def low_keep(v):
    return (low(v), None)

def low_pass(kept, grad):
    return (grad,)

def back_keep(v):
    return (v, None)

def back_low(kept, grad):
    return (low(grad),)
low.defvjp(low_keep, low_pass)
low_back.defvjp(back_keep, back_low)
PRECISE = lax.Precision.HIGHEST
BALANCE_WARMTH = 0.75
EPSILON = 1e-06
FORBIDDEN_AFFINE = -1000000000.0

def layer_norm(values, gain_values, bias_values):
    center = values - lax.optimization_barrier(jnp.mean(values, axis=-1, keepdims=True))
    return center * lax.rsqrt(lax.optimization_barrier(jnp.mean(center * center, axis=-1, keepdims=True)) + EPSILON) * gain_values + bias_values

def log_total(values, axis_number):
    highest = lax.optimization_barrier(jnp.max(values, axis=axis_number, keepdims=True))
    return highest + jnp.log(lax.optimization_barrier(jnp.sum(jnp.exp(values - highest), axis=axis_number, keepdims=True)))

def sort_plan(summary, weights_sort, legal_block_links):
    reorder_affinity = jnp.einsum('rid,dhj->rhij', summary, weights_sort, precision=PRECISE)
    plan_power_factor = jnp.where(legal_block_links, reorder_affinity / BALANCE_WARMTH, FORBIDDEN_AFFINE)
    for balancing_round in range(SINK_ITERS):
        plan_power_factor = plan_power_factor - log_total(plan_power_factor, 3)
        plan_power_factor = plan_power_factor - log_total(plan_power_factor, 2)
    return jnp.exp(plan_power_factor)

def block_masks(segments):
    row_count = segments.shape[0]
    first_segment = segments[:, ::BLOCK]
    last_segment = segments[:, BLOCK - 1::BLOCK]
    block_order = jnp.arange(NBLK)
    diagonal = block_order[:, None] == block_order[None, :]
    earlier = block_order[None, :] < block_order[:, None]
    legal_block_links = diagonal[None] | earlier[None] & (last_segment[:, None, :] == first_segment[:, :, None])
    blocked = segments.reshape(row_count, NBLK, BLOCK)
    position = jnp.arange(BLOCK)
    causal = position[None, :] <= position[:, None]
    same_segment = blocked[:, :, :, None] == blocked[:, :, None, :]
    nearby_pairs = causal[None, None] & same_segment
    visible = jnp.concatenate([nearby_pairs, jnp.ones_like(nearby_pairs)], axis=-1)[:, None]
    return (legal_block_links[:, None], visible)

def layer_forward(inputs, segments, first_gain, first_bias, project_in, sort_weight, project_out, second_gain, second_bias, up_weight, up_bias, down_weight, down_bias):
    row_count = segments.shape[0]
    legal_block_links, visible = block_masks(segments)
    normed_one = low(layer_norm(inputs, first_gain, first_bias))
    projected = low(low_back(jnp.einsum('td,dce->tce', normed_one, project_in, precision=PRECISE)))
    projected = projected.reshape(row_count, NBLK, BLOCK, 3, HEADS, HEAD_DIM)
    question_vectors = projected[:, :, :, 0]
    keys_block = projected[:, :, :, 1]
    values_block = projected[:, :, :, 2]
    summary = lax.optimization_barrier(jnp.mean(normed_one.reshape(row_count, NBLK, BLOCK, D), axis=2))
    plan_matrix = sort_plan(summary, sort_weight, legal_block_links)
    sorted_keys = low(jnp.einsum('rhij,rjshe->rishe', plan_matrix, keys_block, precision=PRECISE))
    sorted_values = low(jnp.einsum('rhij,rjshe->rishe', plan_matrix, values_block, precision=PRECISE))
    keys_joined = jnp.concatenate([keys_block, sorted_keys], axis=2)
    values_joined = jnp.concatenate([values_block, sorted_values], axis=2)
    raw_scores = low_back(jnp.einsum('rithe,rishe->rhits', question_vectors, keys_joined, precision=PRECISE) * HEAD_DIM ** (-0.5))
    scores = jnp.where(visible, raw_scores, FORBIDDEN_AFFINE)
    highest = lax.optimization_barrier(jnp.max(scores, axis=-1, keepdims=True))
    exponent = jnp.exp(scores - highest)
    weights_low = low(exponent / lax.optimization_barrier(jnp.sum(exponent, axis=-1, keepdims=True)))
    mixed_heads = low(low_back(jnp.einsum('rhits,rishe->rithe', weights_low, values_joined, precision=PRECISE)))
    mixed_flat = mixed_heads.reshape(-1, D)
    residual = inputs + low_back(jnp.dot(mixed_flat, project_out, precision=PRECISE))
    normed_two = low(layer_norm(residual, second_gain, second_bias))
    hidden = low_back(jnp.dot(normed_two, up_weight, precision=PRECISE) + up_bias)
    activated = low(jax.nn.gelu(hidden, approximate=True))
    return residual + (jnp.dot(activated, down_weight, precision=PRECISE) + down_bias)

def reference(inputs, segments, cotangent, first_gain, first_bias, project_in, sort_weight, project_out, second_gain, second_bias, up_weight, up_bias, down_weight, down_bias):
    weights_all = tuple((weight_item.astype(jnp.float32) for weight_item in (first_gain, first_bias, project_in, sort_weight, project_out, second_gain, second_bias, up_weight, up_bias, down_weight, down_bias)))
    group_rows = math.gcd(segments.shape[0], 16)
    groups_number = segments.shape[0] // group_rows
    group_tokens = group_rows * LEN
    inputs_groups = inputs.astype(jnp.float32).reshape(groups_number, group_tokens, D)
    cotangent_groups = cotangent.astype(jnp.float32).reshape(groups_number, group_tokens, D)
    segment_groups = segments.reshape(groups_number, group_rows, LEN)

    def group_step(totals, pieces):
        inputs_piece, segment_piece, cotangent_piece = pieces

        def forward_piece(inputs_value, *weights_value):
            return layer_forward(inputs_value, segment_piece, *weights_value)
        result, pullback = jax.vjp(forward_piece, inputs_piece, *weights_all)
        gradients = pullback(cotangent_piece)
        totals = tuple((total_item + grad_item for total_item, grad_item in zip(totals, gradients[1:])))
        return (totals, (result.astype(jnp.bfloat16), gradients[0].astype(jnp.bfloat16)))
    initial = tuple((jnp.zeros_like(weight_item) for weight_item in weights_all))
    totals, (outputs_all, grad_all) = lax.scan(group_step, initial, (inputs_groups, segment_groups, cotangent_groups))
    return (outputs_all.reshape(-1, D), grad_all.reshape(-1, D), totals[0], totals[1], totals[2], totals[3], totals[4], totals[5], totals[6], totals[7], totals[8], totals[9], totals[10])
```

```python
import math

import jax
import jax.numpy as jnp
from jax import lax
from jax.experimental import pallas as pl
from jax.experimental.pallas import tpu as pltpu
from jax.sharding import PartitionSpec as P

HEAD_DIM = 64
BLOCK = 32
NBLK = 8
SINK_ITERS = 8
WARMTH = 0.75
EPSILON = 1e-06
FORBIDDEN = -1000000000.0
GELU_A = math.sqrt(2.0 / math.pi)
GELU_B = 0.044715
MESH = pl.DeviceIdType.MESH
F32, BF16 = jnp.float32, jnp.bfloat16
T, D, PAIR = 256, 512, 128
ROWS = 2048
DOWN, UP, ATT = 0, 1, 2


def nn(a, b):
    return lax.dot_general(a, b, (((1,), (0,)), ((), ())), preferred_element_type=F32)


def nt(a, b):
    return lax.dot_general(a, b, (((1,), (1,)), ((), ())), preferred_element_type=F32)


def tn(a, b):
    return lax.dot_general(a, b, (((0,), (0,)), ((), ())), preferred_element_type=F32)


def precise(a, b, dims):
    return lax.dot_general(
        a, b, (dims, ((), ())), preferred_element_type=F32, precision=lax.Precision.HIGHEST
    )


def iota(shape, dim):
    return lax.broadcasted_iota(jnp.int32, shape, dim)


def parts_of(v, count):
    out = []
    for _ in range(count):
        low = v.astype(BF16)
        out.append(low)
        v = v - low.astype(F32)
    return out


def spin(v, op, axis, shifts):
    for shift in shifts:
        v = op(v, pltpu.roll(v, shift, axis))
    return v


def norm_forward(values, gain, bias):
    center = values - jnp.mean(values, axis=-1, keepdims=True)
    spread = lax.rsqrt(jnp.mean(center * center, axis=-1, keepdims=True) + EPSILON)
    unit = center * spread
    return unit * gain + bias, unit, spread


def norm_backward(upstream, gain, unit, spread):
    through = upstream * gain
    inner = (
        through
        - jnp.mean(through, axis=-1, keepdims=True)
        - unit * jnp.mean(through * unit, axis=-1, keepdims=True)
    )
    return (
        spread * inner,
        jnp.sum(upstream * unit, axis=0, keepdims=True),
        jnp.sum(upstream, axis=0, keepdims=True),
    )


def kernel(
    bits,
    x_ref, seg_ref, cot_ref, g1_ref, b1_ref, g2_ref, b2_ref, db_ref,
    win_h, wout_h, misc_h, wup_h, wdn_h,
    out_ref, gx_ref, fin_ref, small_ref,
    win, wout, misc, wup, wdn,
    swp, unit1, spread1, n1_ref, q_ref, kj_ref, vj_ref, steps, pe_ref, prob_ref, mix_ref,
    res_ref, n2_ref, unit2, spread2, y_ref, gn2_ref, gres_ref, gm_ref, gn1_ref, gt_ref,
    gkj_ref, gvj_ref, gp_ref, gs_ref, vis_ref, bm_ref,
    gloc, rcore, ryy, rdp, sloc, srec_c, srec_y, sacc, srec_d, vec,
    lsem, wsend, wrecv, csend, crecv, ysend, yrecv, dsend, drecv, asend, arecv, ssend, srecv,
):
    dp, h = lax.axis_index("dp"), lax.axis_index("head")
    hb0, hb1 = lax.rem(h, 2), h // 2
    step_c, step_y = 1 - 2 * hb0, 2 - 4 * hb1
    core = {"dp": dp, "head": h + step_c}
    ydev = {"dp": dp, "head": h + step_y}
    bit = [lax.rem(dp // (1 << b), 2) for b in range(bits)]
    dpdev = [{"dp": dp + (1 << b) * (1 - 2 * bit[b]), "head": h} for b in range(bits)]
    xb, xdev = bit[0], dpdev[0]

    def shard(o):
        return h + (1 - lax.rem(o, 2)) * step_c + (1 - o // 2) * step_y

    def remote(src, dst, send, recv, dev):
        return pltpu.make_async_remote_copy(
            src_ref=src, dst_ref=dst, send_sem=send, recv_sem=recv, device_id=dev, device_id_type=MESH
        )

    barrier = pltpu.get_barrier_semaphore()
    for dev in [core, ydev] + dpdev:
        pl.semaphore_signal(barrier, inc=1, device_id=dev, device_id_type=MESH)
    pl.semaphore_wait(barrier, 2 + bits)

    weights = [(win_h, win), (misc_h, misc), (wout_h, wout), (wup_h, wup), (wdn_h, wdn)]
    opposite = h + step_y
    local, w_core, w_y, w_x, w_c1, w_c2 = [], [], [], [], [], []
    for a, (src, full) in enumerate(weights):
        half = src.shape[0] // 2
        mine = pl.ds(pl.multiple_of(xb * half, half), half)
        other = pl.ds(pl.multiple_of((1 - xb) * half, half), half)
        local.append(pltpu.make_async_copy(src, full.at[h], lsem.at[a]))
        w_core.append(remote(src, full.at[h], wsend.at[a, 0], wrecv.at[a, 0], core))
        w_y.append(remote(src.at[mine], full.at[h, mine], wsend.at[a, 1], wrecv.at[a, 1], ydev))
        got, late = full.at[opposite, mine], full.at[opposite, other]
        w_x.append(remote(got, got, wsend.at[a, 2], wrecv.at[a, 2], xdev))
        w_c1.append(remote(got, got, wsend.at[a, 3], wrecv.at[a, 3], core))
        w_c2.append(remote(late, late, wsend.at[a, 4], wrecv.at[a, 4], core))
    for a in range(5):
        w_y[a].start()
        w_core[a].start()
        local[a].start()

    def relay_y(a):
        w_y[a].wait_recv()
        w_x[a].start()
        w_c1[a].start()

    def relay_x(a):
        w_x[a].wait_recv()
        w_c2[a].start()

    def arrived(a):
        local[a].wait()
        w_core[a].wait_recv()
        w_c1[a].wait_recv()
        w_c2[a].wait_recv()

    x = x_ref[...].astype(F32)
    normed, unit, spread = norm_forward(x, g1_ref[...], b1_ref[...])
    unit1[...] = unit
    spread1[...] = spread
    n1_ref[...] = normed.astype(BF16)
    blk_row, blk_lane = iota((T, T), 0) // BLOCK, iota((T, T), 1) // BLOCK
    bm_ref[...] = jnp.where(blk_row == blk_lane, 1.0, 0.0).astype(BF16)
    seg8 = jnp.broadcast_to(seg_ref[pl.ds(h, 1), :].astype(F32), (8, T))
    eye = jnp.where(iota((T, T), 0) == iota((T, T), 1), 1.0, 0.0).astype(BF16)
    seg_col = nt(eye, seg8.astype(BF16))[:, :1]
    lane_blk = iota((BLOCK, T), 1) // BLOCK

    def pick(full):
        acc = full[:BLOCK]
        for j in range(1, NBLK):
            acc = jnp.where(lane_blk == j, full[j * BLOCK : (j + 1) * BLOCK], acc)
        return acc

    seg_key = pick(jnp.broadcast_to(seg_col, (T, T)))
    causal = iota((BLOCK, T), 0) <= lax.rem(iota((BLOCK, T), 1), BLOCK)
    vis_ref[...] = jnp.where(causal & (seg_key == seg8[:1]), 1.0, 0.0)

    relay_y(0)
    relay_y(1)
    relay_x(0)
    relay_x(1)
    arrived(0)

    def project(s, carry):
        r = nn(n1_ref[...], win[s]).astype(BF16)
        q_ref[s] = r[:, :PAIR]
        kj_ref[s, :T] = r[:, PAIR : 2 * PAIR]
        vj_ref[s, :T] = r[:, 2 * PAIR :]
        return carry

    lax.fori_loop(0, 4, project, 0)
    relay_y(2)
    relay_x(2)
    relay_y(3)
    arrived(1)

    for s in range(4):
        for hl in range(2):
            for c in range(4):
                rows = misc[s, hl * 8 : hl * 8 + 8, c * PAIR : (c + 1) * PAIR]
                swp[c, pl.ds(2 * s + hl, 8, stride=8), :] = rows
                swp[c, pl.ds(64 + 2 * s + hl, 8, stride=8), :] = rows
    sorter = jnp.concatenate([swp[c] for c in range(4)], axis=1)
    averager = jnp.where(iota((NBLK, T), 0) == iota((NBLK, T), 1) // BLOCK, 1.0 / BLOCK, 0.0).astype(BF16)
    summary = nn(averager, n1_ref[...])
    logits = precise(summary, sorter, ((1,), (1,)))
    row_i, lane_j = iota((8, PAIR), 0), lax.rem(iota((8, PAIR), 1), 64) // 8
    first_seg = jnp.sum(jnp.where(iota((8, T), 1) == BLOCK * iota((8, T), 0), seg8, 0.0), axis=1, keepdims=True)
    last_of = jnp.where(
        iota((PAIR, T), 1) == BLOCK * (lax.rem(iota((PAIR, T), 0), 64) // 8) + BLOCK - 1, 1.0, 0.0
    ).astype(BF16)
    last_seg = nt(seg8.astype(BF16), last_of)
    allowed = (lane_j == row_i) | ((lane_j < row_i) & (first_seg == last_seg))
    z = jnp.where(allowed, logits / WARMTH, FORBIDDEN)
    ways = [(1, (8, 16, 32)), (0, (1, 2, 4))]
    for it in range(2 * SINK_ITERS):
        axis, shifts = ways[it % 2]
        highest = spin(z, jnp.maximum, axis, shifts)
        e = jnp.exp(z - highest)
        total = spin(e, jnp.add, axis, shifts)
        steps[it] = e / total
        z = z - (highest + jnp.log(total))
    plan = jnp.exp(z)
    expand = jnp.where(lax.rem(iota((PAIR, D), 0), 8) == iota((PAIR, D), 1) // HEAD_DIM, 1.0, 0.0).astype(BF16)
    lane_full = iota((8, PAIR), 1) // 8
    spreadout = jnp.concatenate([jnp.where(lane_full == j, plan, 0.0) for j in range(NBLK)], axis=0)
    pe = sum(nn(part, expand) for part in parts_of(spreadout, 3))
    for s in range(4):
        pe_ref[s] = pe[:, s * PAIR : (s + 1) * PAIR]

    lane = iota((1, PAIR), 1)
    vis = vis_ref[...] > 0.5

    def mask_of(a):
        return jnp.where(lane // HEAD_DIM == a, 1.0, 0.0).astype(BF16)

    def block_diag(p):
        low = p.astype(BF16)
        return jnp.concatenate([low] * NBLK, axis=0) * bm_ref[...]

    def sort_rows(s, i):
        acc_k = jnp.zeros((BLOCK, PAIR), F32)
        acc_v = jnp.zeros((BLOCK, PAIR), F32)
        for j in range(NBLK):
            p = pe_ref[s, pl.ds(j * 8 + i, 1), :]
            acc_k += p * kj_ref[s, j * BLOCK : (j + 1) * BLOCK, :].astype(F32)
            acc_v += p * vj_ref[s, j * BLOCK : (j + 1) * BLOCK, :].astype(F32)
        at = pl.ds(pl.multiple_of(T + i * BLOCK, BLOCK), BLOCK)
        kj_ref[s, at, :] = acc_k.astype(BF16)
        vj_ref[s, at, :] = acc_v.astype(BF16)

    def attend(s, carry):
        def one(i, c):
            sort_rows(s, i)
            return c

        lax.fori_loop(0, NBLK, one, 0)
        q, kj, vj = q_ref[s], kj_ref[s], vj_ref[s]
        mixed = jnp.zeros((T, PAIR), F32)
        for a in range(2):
            full = nt(kj, q * mask_of(a)) * (HEAD_DIM**-0.5)
            own = jnp.where(vis, pick(full[:T]), FORBIDDEN)
            far = pick(full[T:])
            highest = jnp.maximum(jnp.max(own, axis=0, keepdims=True), jnp.max(far, axis=0, keepdims=True))
            own, far = jnp.exp(own - highest), jnp.exp(far - highest)
            inverse = 1.0 / (jnp.sum(own, axis=0, keepdims=True) + jnp.sum(far, axis=0, keepdims=True))
            own, far = own * inverse, far * inverse
            prob_ref[2 * s + a, :BLOCK] = own
            prob_ref[2 * s + a, BLOCK:] = far
            vm = vj * mask_of(a)
            mixed += tn(block_diag(own), vm[:T]) + tn(block_diag(far), vm[T:])
        mix_ref[:, pl.ds(pl.multiple_of(s * PAIR, PAIR), PAIR)] = mixed.astype(BF16)
        return carry

    lax.fori_loop(0, 2, attend, 0)
    relay_x(3)
    relay_y(4)
    lax.fori_loop(2, 4, attend, 0)
    relay_x(4)
    arrived(2)
    wout_all = wout[...].reshape(D, D)
    residual = x_ref[...].astype(F32) + nn(mix_ref[...], wout_all)
    res_ref[...] = residual
    normed, unit, spread = norm_forward(residual, g2_ref[...], b2_ref[...])
    unit2[...] = unit
    spread2[...] = spread
    n2_ref[...] = normed.astype(BF16)
    vec[...] = jnp.zeros_like(vec)
    y_ref[...] = jnp.zeros_like(y_ref)
    gn2_ref[...] = jnp.zeros_like(gn2_ref)
    arrived(3)
    arrived(4)

    c_copy = [
        [remote(gloc.at[2 * w, k], rcore.at[w, k], csend.at[w, k], crecv.at[w, k], core) for k in range(3)]
        for w in range(2)
    ]
    y_copy = [remote(gloc.at[1, k], ryy.at[k], ysend.at[k], yrecv.at[k], ydev) for k in range(3)]
    down_copy, up_copy, spans = [], [], []
    for k in range(3):
        off, n = 0, ROWS
        downs, ups, keeps = [], [], []
        for b in range(bits):
            n //= 2
            keep, give = off + bit[b] * n, off + (1 - bit[b]) * n
            downs.append(
                remote(
                    gloc.at[3, k, pl.ds(pl.multiple_of(give, n), n)], rdp.at[k, pl.ds(n, n)],
                    dsend.at[k, b], drecv.at[k, b], dpdev[b],
                )
            )
            here = fin_ref.at[k, pl.ds(pl.multiple_of(keep, n), n)]
            ups.append(remote(here, here, asend.at[k, b], arecv.at[k, b], dpdev[b]))
            keeps.append((keep, n))
            off = keep
        down_copy.append(downs)
        up_copy.append(ups)
        spans.append(keeps)

    def summed(dst, terms, n):
        size = min(n, 256)

        def body(i, c):
            at = pl.ds(pl.multiple_of(i * size, size), size)
            v = terms[0][at, :].astype(F32)
            for term in terms[1:]:
                v += term[at, :].astype(F32)
            dst[at, :] = v.astype(BF16)
            return c

        lax.fori_loop(0, n // size, body, 0)

    def exchange(o, chunks):
        @pl.when(o == 0)
        def _():
            for k in chunks:
                c_copy[0][k].start()

        @pl.when(o == 1)
        def _():
            for k in chunks:
                c_copy[0][k].wait_recv()
                summed(gloc.at[1, k], [gloc.at[1, k], rcore.at[0, k]], ROWS)
                y_copy[k].start()

        @pl.when(o == 2)
        def _():
            for k in chunks:
                c_copy[1][k].start()

    def stage(k, t):
        if t == 0:
            c_copy[1][k].wait_recv()
            y_copy[k].wait_recv()
            summed(gloc.at[3, k], [gloc.at[3, k], rcore.at[1, k], ryy.at[k]], ROWS)
            down_copy[k][0].start()
        elif t <= bits:
            down_copy[k][t - 1].wait()
            keep, n = spans[k][t - 1]
            at = pl.ds(pl.multiple_of(keep, n), n)
            region = gloc.at[3, k, at]
            summed(region if t < bits else fin_ref.at[k, at], [region, rdp.at[k, pl.ds(n, n)]], n)
            if t < bits:
                down_copy[k][t].start()
            else:
                up_copy[k][bits - 1].start()
        else:
            up_copy[k][2 * bits - t].wait()
            if t < 2 * bits:
                up_copy[k][2 * bits - t - 1].start()

    def put_square(o, k, value, base, height):
        for c in range(value.shape[1] // PAIR):
            gloc[o, k, base + c * height : base + (c + 1) * height, :] = value[
                :, c * PAIR : (c + 1) * PAIR
            ].astype(BF16)

    def feed(o, carry):
        ss = shard(o)
        n2, cot = n2_ref[...], cot_ref[...]
        w_up, w_dn = wup[ss], wdn[ss]
        v = nn(n2, w_up) + misc[ss, 16:17, :]
        square = v * v
        th = jnp.tanh(GELU_A * v * (1.0 + GELU_B * square))
        act = (0.5 * v * (1.0 + th)).astype(BF16)
        slope = 0.5 * (1.0 + th) + 0.5 * v * (1.0 - th * th) * (GELU_A * (1.0 + 3.0 * GELU_B * square))
        grad = nt(cot, w_dn) * slope
        gh = grad.astype(BF16)
        y_ref[...] += nn(act, w_dn)
        put_square(o, DOWN, tn(act, cot), 0, D)
        put_square(o, UP, tn(n2, gh), 0, D)
        vec[pl.ds(5 + ss, 1), :] = jnp.sum(gh.astype(F32), axis=0, keepdims=True)
        gn2_ref[...] += nt(gh, w_up)
        exchange(o, (DOWN, UP))
        return carry

    lax.fori_loop(0, 4, feed, 0)
    out_ref[...] = (res_ref[...] + (y_ref[...] + db_ref[...])).astype(BF16)

    cot = cot_ref[...].astype(F32)
    back, gain, bias = norm_backward(gn2_ref[...], g2_ref[...], unit2[...], spread2[...])
    vec[2:3, :] = gain
    vec[3:4, :] = bias
    vec[4:5, :] = jnp.sum(cot, axis=0, keepdims=True)
    gres = cot + back
    gres_ref[...] = gres
    branch = gres.astype(BF16)
    gm_ref[...] = nt(branch, wout_all).astype(BF16)
    for o in range(4):
        at = pl.ds(pl.multiple_of(shard(jnp.int32(o)) * PAIR, PAIR), PAIR)
        put_square(o, ATT, tn(mix_ref[:, at], branch), 1536, PAIR)
    gn1_ref[...] = jnp.zeros_like(gn1_ref)

    def unattend(o, carry):
        s = shard(o)
        q, kj, vj = q_ref[s], kj_ref[s], vj_ref[s]
        gm = gm_ref[:, pl.ds(pl.multiple_of(s * PAIR, PAIR), PAIR)]
        gq = jnp.zeros((T, PAIR), F32)
        for a in range(2):
            mask = mask_of(a)
            gmm, qm, km = gm * mask, q * mask, kj * mask
            full = nt(vj, gmm)
            g_own, g_far = pick(full[:T]), pick(full[T:])
            own, far = prob_ref[2 * s + a, :BLOCK], prob_ref[2 * s + a, BLOCK:]
            dot = jnp.sum(g_own * own, axis=0, keepdims=True) + jnp.sum(g_far * far, axis=0, keepdims=True)
            s_own, s_far = block_diag(own * (g_own - dot)), block_diag(far * (g_far - dot))
            v_own, v_far = nn(block_diag(own), gmm), nn(block_diag(far), gmm)
            k_own, k_far = nn(s_own, qm), nn(s_far, qm)
            gq += tn(s_own, km[:T]) + tn(s_far, km[T:])
            if a == 0:
                gvj_ref[:T], gvj_ref[T:] = v_own, v_far
                gkj_ref[:T], gkj_ref[T:] = k_own, k_far
            else:
                gvj_ref[:T] += v_own
                gvj_ref[T:] += v_far
                gkj_ref[:T] = (gkj_ref[:T] + k_own) * (HEAD_DIM**-0.5)
                gkj_ref[T:] = (gkj_ref[T:] + k_far) * (HEAD_DIM**-0.5)
        gt_ref[:, :PAIR] = (gq * (HEAD_DIM**-0.5)).astype(BF16)

        def unsort(j, c):
            at = pl.ds(pl.multiple_of(j * BLOCK, BLOCK), BLOCK)
            kb, vb = kj_ref[s, at, :].astype(F32), vj_ref[s, at, :].astype(F32)
            gk, gv = gkj_ref[at, :], gvj_ref[at, :]
            rows = []
            for i in range(NBLK):
                p = pe_ref[s, pl.ds(j * 8 + i, 1), :]
                sk = gkj_ref[T + i * BLOCK : T + (i + 1) * BLOCK, :]
                sv = gvj_ref[T + i * BLOCK : T + (i + 1) * BLOCK, :]
                gk += p * sk
                gv += p * sv
                rows.append(jnp.sum(sk * kb + sv * vb, axis=0, keepdims=True))
            gp_ref[s, pl.ds(pl.multiple_of(j * 8, 8), 8), :] = jnp.concatenate(rows, axis=0)
            gt_ref[at, PAIR : 2 * PAIR] = gk.astype(BF16)
            gt_ref[at, 2 * PAIR :] = gv.astype(BF16)
            return c

        lax.fori_loop(0, NBLK, unsort, 0)
        gt = gt_ref[...]
        put_square(o, ATT, tn(n1_ref[...], gt), 0, D)
        gn1_ref[...] += nt(gt, win[s])
        exchange(o, (ATT,))
        return carry

    lax.fori_loop(0, 4, unattend, 0)

    stage(DOWN, 0)
    gp = jnp.concatenate([gp_ref[s] for s in range(4)], axis=1)
    wide = sum(nt(part, expand) for part in parts_of(gp, 3))
    grad = jnp.zeros((8, PAIR), F32)
    for j in range(NBLK):
        grad = jnp.where(lane_j == j, wide[j * 8 : (j + 1) * 8], grad)
    grad = grad * plan
    for it in reversed(range(2 * SINK_ITERS)):
        axis, shifts = ways[it % 2]
        grad = grad - steps[it] * spin(grad, jnp.add, axis, shifts)
    grad = jnp.where(allowed & (iota((8, PAIR), 1) < 64), grad, 0.0) / WARMTH
    grad_sort = precise(grad, summary, ((0,), (0,)))
    for c in range(4):
        gs_ref[c] = grad_sort[:, c * PAIR : (c + 1) * PAIR]
    sorter = jnp.concatenate([swp[c] for c in range(4)], axis=1)
    grad_summary = precise(grad, sorter, ((1,), (0,))) * (1.0 / BLOCK)
    for place, o in ((0, 0), (1, 2), (3, 1), (4, 3)):
        ss = shard(jnp.int32(o))
        for hl in range(2):
            for c in range(4):
                at = slice(place * 16 + hl * 8, place * 16 + hl * 8 + 8)
                sloc[at, c * PAIR : (c + 1) * PAIR] = gs_ref[c, pl.ds(2 * ss + hl, 8, stride=8), :]
    stage(UP, 0)
    stage(DOWN, 1)

    for i in range(NBLK):
        gn1_ref[i * BLOCK : (i + 1) * BLOCK, :] += grad_summary[i : i + 1, :]
    back, gain, bias = norm_backward(gn1_ref[...], g1_ref[...], unit1[...], spread1[...])
    vec[0:1, :] = gain
    vec[1:2, :] = bias
    gx_ref[...] = (gres_ref[...] + back).astype(BF16)
    sloc[32:48, :] = vec[...]

    small_c = remote(sloc.at[0:48], srec_c, ssend.at[0], srecv.at[0], core)
    small_c.start()
    stage(DOWN, 2)
    stage(UP, 1)
    small_c.wait_recv()
    sloc[48:64, :] += srec_c[0:16, :]
    sloc[64:80, :] += srec_c[16:32, :]
    small_c.wait_send()
    sloc[32:48, :] += srec_c[32:48, :]
    small_y = remote(sloc.at[32:64], srec_y, ssend.at[1], srecv.at[1], ydev)
    small_y.start()
    stage(DOWN, 3)
    stage(UP, 2)
    stage(ATT, 0)
    small_y.wait_recv()
    sacc[0, :16] = sloc[32:48, :] + srec_y[:16, :]
    sacc[0, 16:] = sloc[64:80, :] + srec_y[16:, :]
    small_d = [
        remote(sacc.at[b], srec_d.at[b], ssend.at[2 + b], srecv.at[2 + b], dpdev[b]) for b in range(bits)
    ]
    small_d[0].start()
    last = 2 * bits
    for t in range(1, last + 1):
        if t + 3 <= last:
            stage(DOWN, t + 3)
        if t + 2 <= last:
            stage(UP, t + 2)
        stage(ATT, t)
        if t <= bits:
            small_d[t - 1].wait_recv()
            value = sacc[t - 1] + srec_d[t - 1]
            if t < bits:
                sacc[t] = value
                small_d[t].start()
            else:
                vec[...] = value[:16]
                small_ref[0:5, :] = vec[0:5, :]
                small_ref[5:6, :] = vec[pl.ds(5 + h, 1), :]
                small_ref[6:8, :] = jnp.zeros((2, D), F32)
                small_ref[8:24, :] = value[16:]
    for a in range(5):
        for copy in (w_core[a], w_y[a], w_x[a], w_c1[a], w_c2[a]):
            copy.wait_send()
    for k in range(3):
        c_copy[0][k].wait_send()
        c_copy[1][k].wait_send()
        y_copy[k].wait_send()
    small_y.wait_send()
    for b in range(bits):
        small_d[b].wait_send()


def shards(
    bits, inputs, segments, cotangent, first_gain, first_bias, project_in, sort_weight, project_out,
    second_gain, second_bias, up_weight, up_bias, down_weight, down_bias,
):
    row = lambda v: v.reshape(1, D)
    misc = jnp.concatenate(
        [sort_weight.transpose(1, 2, 0).reshape(16, D), row(up_bias), jnp.zeros((15, D), F32)], axis=0
    )
    vmem, anywhere = pl.BlockSpec(memory_space=pltpu.VMEM), pl.BlockSpec(memory_space=pl.ANY)
    V, dma = pltpu.VMEM, pltpu.SemaphoreType.DMA
    scratch = [
        V((4, D, 384), BF16), V((4, PAIR, D), BF16), V((4, 32, D), F32), V((4, D, D), BF16), V((4, D, D), BF16),
        V((4, PAIR, PAIR), F32), V((T, D), F32), V((T, 1), F32), V((T, D), BF16), V((4, T, PAIR), BF16),
        V((4, 2 * T, PAIR), BF16), V((4, 2 * T, PAIR), BF16), V((2 * SINK_ITERS, 8, PAIR), F32),
        V((4, 64, PAIR), F32), V((8, 64, T), F32), V((T, D), BF16),
        V((T, D), F32), V((T, D), BF16), V((T, D), F32), V((T, 1), F32), V((T, D), F32), V((T, D), F32),
        V((T, D), F32), V((T, D), BF16), V((T, D), F32), V((T, 384), BF16),
        V((2 * T, PAIR), F32), V((2 * T, PAIR), F32), V((4, 64, PAIR), F32), V((4, PAIR, PAIR), F32),
        V((BLOCK, T), F32), V((T, T), BF16),
        V((4, 3, ROWS, PAIR), BF16), V((2, 3, ROWS, PAIR), BF16), V((3, ROWS, PAIR), BF16), V((3, ROWS, PAIR), BF16),
        V((80, D), F32), V((48, D), F32), V((32, D), F32), V((bits, 32, D), F32), V((bits, 32, D), F32), V((16, D), F32),
        dma((5,)), dma((5, 5)), dma((5, 5)), dma((2, 3)), dma((2, 3)), dma((3,)), dma((3,)),
        dma((3, bits)), dma((3, bits)), dma((3, bits)), dma((3, bits)), dma((2 + bits,)), dma((2 + bits,)),
    ]
    out, grad_inputs, fin, small = pl.pallas_call(
        lambda *refs: kernel(bits, *refs),
        name="layer",
        out_shape=(
            jax.ShapeDtypeStruct((T, D), BF16),
            jax.ShapeDtypeStruct((T, D), BF16),
            jax.ShapeDtypeStruct((3, ROWS, PAIR), BF16),
            jax.ShapeDtypeStruct((24, D), F32),
        ),
        in_specs=[vmem] * 8 + [anywhere] * 5,
        out_specs=(vmem,) * 4,
        scratch_shapes=scratch,
        compiler_params=pltpu.CompilerParams(
            collective_id=0, has_side_effects=True, vmem_limit_bytes=60 * 1024 * 1024
        ),
    )(
        inputs, segments, cotangent, row(first_gain), row(first_bias), row(second_gain), row(second_bias),
        row(down_bias), project_in.reshape(D, 384), project_out, misc, up_weight, down_weight,
    )

    def square(v, height):
        return v.reshape(-1, height, PAIR).transpose(1, 0, 2).reshape(height, -1).astype(F32)

    return (
        out,
        grad_inputs,
        small[0],
        small[1],
        fin[ATT, :1536].reshape(3, D, PAIR).transpose(1, 0, 2).astype(F32),
        small[8:24].reshape(2, 8, D).transpose(2, 0, 1),
        square(fin[ATT, 1536:], PAIR),
        small[2],
        small[3],
        square(fin[UP], D),
        small[5],
        square(fin[DOWN], D),
        small[4],
    )


def solution(mesh):
    bits = mesh.shape["dp"].bit_length() - 1
    rows = P(("dp", "head"), None)
    return jax.shard_map(
        lambda *args: shards(bits, *args),
        mesh=mesh,
        in_specs=(
            rows, P("dp", None), rows, P(), P(), P(None, None, "head"), P(None, "head", None),
            P("head", None), P(), P(), P(None, "head"), P("head"), P("head", None), P(),
        ),
        out_specs=(
            rows, rows, P(), P(), P(None, None, "head"), P(None, "head", None), P("head", None),
            P(), P(), P(None, "head"), P("head"), P("head", None), P(),
        ),
        check_vma=False,
    )
```
